32 devices in a mesh: blk: 16 (over z, x, core), rep: 2 (over y).
Axes of the slice: x: 2, y: 2, z: 4, core: 2. Of those that a mesh axis runs over, the one named last changes fastest.
Arguments:
- captions: bfloat16 [6144, 768], P(('blk', 'rep')), may hold values from -512 to 512
- images: bfloat16 [6144, 768], P(('blk', 'rep')), may hold values from -512 to 512
- positives: int32 [6144], P(('blk', 'rep')), may hold values from 0 to 6143, each once
- valid: int32 [6144], P(('blk', 'rep')), may hold values from 0 to 1, as said below
Outputs:
- caption_loss: float32 [6144], P(('blk', 'rep'))
- image_loss: float32 [6144], P(('blk', 'rep'))
- loss: float32 [], replicated
The draws below stay inside these ranges and needn't reach their ends.
Inputs may be any that keep to these rules, and one draw needn't show every extreme that they name: `positives`: each image row is the positive of exactly one caption; a program may pack several of these indices into one sent element. `valid`: the last image row is always real; a program may pack several of these flags into one sent element.
All inputs are finite; a program needn't handle non-finite values.
Results may differ from the reference program's by a relative error of at most 0.0003.
Values may be sent and summed in bfloat16 or wider, within the bound.
A program may use at most 128 MiB of HBM per device.

```python
import math
import jax
import jax.numpy as jnp
from jax import lax

E = 768
PAIRS = 6144


def pair_fields(key):
    base_key = jax.random.fold_in(key, 11)
    caption_key, image_key = jax.random.split(base_key, 2)
    caption_rows = jax.random.normal(caption_key, (PAIRS, E), jnp.float32)
    image_rows = jax.random.normal(image_key, (PAIRS, E), jnp.float32) * (3.0 / math.sqrt(E))
    return (caption_rows.astype(jnp.bfloat16), image_rows.astype(jnp.bfloat16))


def draw_captions(key, part):
    return pair_fields(key)[0]


def draw_images(key, part):
    return pair_fields(key)[1]


def draw_valid(key, part):
    position = jax.lax.iota(jnp.int32, PAIRS)
    rolled = jax.random.randint(jax.random.fold_in(key, 23), (PAIRS,), 0, 4 * PAIRS)
    flags = (rolled < PAIRS + 2 * position).astype(jnp.int32)
    return flags.at[PAIRS - 1].set(1)


def setup_inputs(seed: int = 0) -> dict:
    keys = jax.random.split(jax.random.key(seed), 5)
    captions = draw_captions(jax.random.fold_in(keys[4], 71), 0)
    images = draw_images(jax.random.fold_in(keys[4], 71), 0)
    positives = jax.random.permutation(keys[2], PAIRS).astype(jnp.int32)
    valid = draw_valid(jax.random.fold_in(keys[4], 71), 0)
    return {"captions": captions, "images": images, "positives": positives, "valid": valid}


very_low = -1.0e30


def reference(captions, images, positives, valid):
    pair_count = captions.shape[0]
    block_size = math.gcd(pair_count, 1024)
    image_ok = valid.astype(jnp.float32)
    caption_ok = jnp.take(image_ok, positives, axis=0)
    usable = image_ok[None, :] > 0
    columns = lax.iota(jnp.int32, pair_count)

    def one_block(running, block_index):
        column_peak, column_total, column_match = running
        offset = (block_index * block_size).astype(jnp.int32)
        caption_rows = lax.dynamic_slice_in_dim(captions, offset, block_size)
        match_rows = lax.dynamic_slice_in_dim(positives, offset, block_size)
        ok_rows = lax.dynamic_slice_in_dim(caption_ok, offset, block_size)
        scores = jnp.dot(caption_rows, images.T, preferred_element_type=jnp.float32)
        is_positive = match_rows[:, None] == columns[None, :]
        picked = jnp.where(is_positive, scores, 0.0)
        highest = jnp.max(jnp.where(usable, scores, very_low), axis=1)
        row_total = jnp.sum(jnp.where(usable, jnp.exp(scores - highest[:, None]), 0.0), axis=1)
        row_loss = ok_rows * (highest + jnp.log(row_total) - jnp.sum(picked, axis=1))
        caption_live = ok_rows[:, None] > 0
        column_high = jnp.max(jnp.where(caption_live, scores, very_low), axis=0)
        renewed = jnp.maximum(column_peak, column_high)
        powers = jnp.where(caption_live, jnp.exp(scores - renewed[None, :]), 0.0)
        column_total = column_total * jnp.exp(column_peak - renewed) + jnp.sum(powers, axis=0)
        column_match = column_match + jnp.sum(picked, axis=0)
        return (renewed, column_total, column_match), row_loss

    started = (jnp.full((pair_count,), very_low, jnp.float32), jnp.zeros((pair_count,), jnp.float32), jnp.zeros((pair_count,), jnp.float32))
    finished, row_losses = lax.scan(one_block, started, jnp.arange(pair_count // block_size, dtype=jnp.int32))
    caption_loss = row_losses.reshape(pair_count)
    image_loss = image_ok * (finished[0] + jnp.log(finished[1]) - finished[2])
    loss = (jnp.sum(caption_loss) + jnp.sum(image_loss)) / (2.0 * jnp.sum(image_ok))
    return (caption_loss, image_loss, loss)
```

```python
import functools

import jax
import jax.numpy as jnp
from jax import lax
from jax.experimental import pallas as pl
from jax.experimental.pallas import tpu as pltpu
from jax.sharding import PartitionSpec as P

very_low = -1e30
floor = -1e29
PIECES = 2


def grid_of(blk, rep):
    chips = (blk // 2) * rep
    planes = 1
    while (planes * 2) ** 2 <= chips and (blk // 2) % (planes * 2) == 0:
        planes *= 2
    return planes, blk // 2 // planes


def kernel(
    blk, rep, cap_ref, img_ref, pos_ref, val_ref, closs_ref, iloss_ref, loss_ref,
    caps, imgs, posb, vbuf, rowsend, rowrecv, colsend, colrecv, part, colacc,
    loc_sem, up_sem, down_sem, cap_sem, pos_send, pos_recv, val_send, val_recv,
    own_send, relay_send, img_sem, row_send, row_recv, col_send, col_recv, part_send, part_recv,
):
    U, V = grid_of(blk, rep)
    N = blk * rep
    G = N // U
    n = cap_ref.shape[0]
    ph = n // PIECES
    b, r = lax.axis_index("blk"), lax.axis_index("rep")
    core = b % 2
    u = b // (2 * V)
    v = (b // 2) % V
    me = b * rep + r
    g = me % G

    def member(uu, gg):
        return {"blk": uu * (2 * V) + gg // rep, "rep": gg % rep}

    def device(index):
        return {"blk": index // rep, "rep": index % rep}

    def remote(src, dst, ss, rs, to):
        return pltpu.make_async_remote_copy(
            src_ref=src, dst_ref=dst, send_sem=ss, recv_sem=rs, device_id=to,
            device_id_type=pl.DeviceIdType.MESH,
        )

    barrier = pltpu.get_barrier_semaphore()

    @pl.loop(1, N)
    def _(k):
        pl.semaphore_signal(
            barrier, inc=1, device_id=device((me + k) % N), device_id_type=pl.DeviceIdType.MESH
        )

    pl.semaphore_wait(barrier, N - 1)

    def cap_copy(slot, p, up):
        rows = pl.ds(p * ph, ph)
        to = member(u + 1 if up else u - 1, g)
        return remote(
            caps.at[slot, rows], caps.at[slot, rows],
            (up_sem if up else down_sem).at[slot * PIECES + p], cap_sem.at[slot * PIECES + p], to,
        )

    def own_cap_copy(p, up):
        rows = pl.ds(p * ph, ph)
        to = member(u + 1 if up else u - 1, g)
        return remote(
            cap_ref.at[rows], caps.at[u, rows],
            (up_sem if up else down_sem).at[u * PIECES + p], cap_sem.at[u * PIECES + p], to,
        )

    for p in range(PIECES):
        @pl.when(u < U - 1)
        def _():
            own_cap_copy(p, True).start()

        @pl.when(u > 0)
        def _():
            own_cap_copy(p, False).start()

    def same_core(k):
        vv, rr = (v + k // rep) % V, (r + k % rep) % rep
        return (vv * 2 + core) * rep + rr

    partner = (v * 2 + 1 - core) * rep + r
    M = V * rep

    def own_img_copy(k):
        to = partner if k == 0 else same_core(k)
        return remote(img_ref, imgs.at[g], own_send.at[k], img_sem.at[g], member(u, to))

    def relay_copy(k):
        slot = same_core(k)
        return remote(
            imgs.at[slot], imgs.at[slot], relay_send.at[k], img_sem.at[slot], member(u, partner)
        )

    for k in list(range(1, M)) + [0]:
        own_img_copy(k).start()

    def pos_copy(k):
        return remote(
            pos_ref, posb.at[u], pos_send.at[k], pos_recv.at[u], member((u + k) % U, g)
        )

    for k in range(1, U):
        pos_copy(k).start()

    def val_copy(k):
        return remote(
            val_ref, vbuf.at[me], val_send.at[k], val_recv.at[me], device((me + k) % N)
        )

    @pl.loop(1, N)
    def _(k):
        val_copy(k).start()

    cap_local = pltpu.make_async_copy(cap_ref, caps.at[u], loc_sem.at[0])
    img_local = pltpu.make_async_copy(img_ref, imgs.at[g], loc_sem.at[1])
    cap_local.start()
    img_local.start()
    posb[u] = pos_ref[...]
    vbuf[me] = val_ref[...]

    def pass_on(distance):
        for p in range(PIECES):
            @pl.when(u - distance >= 0)
            def _():
                copy = cap_copy(u - distance, p, True)
                copy.wait_recv()

                @pl.when(u < U - 1)
                def _():
                    copy.start()

            @pl.when(u + distance < U)
            def _():
                copy = cap_copy(u + distance, p, False)
                copy.wait_recv()

                @pl.when(u > 0)
                def _():
                    copy.start()

    @pl.loop(1, N)
    def _(k):
        slot = (me + k) % N
        remote(
            val_ref, vbuf.at[slot], val_send.at[k], val_recv.at[slot], device(slot)
        ).wait_recv()

    for k in range(1, U):
        slot = (u + k) % U
        remote(
            pos_ref, posb.at[slot], pos_send.at[k], pos_recv.at[slot], member(slot, g)
        ).wait_recv()

    eye = lax.broadcasted_iota(jnp.int32, (n, n), 0) == lax.broadcasted_iota(jnp.int32, (n, n), 1)

    def to_column(row):
        return jnp.sum(jnp.where(eye, row, 0.0), axis=1, keepdims=True)

    def to_row(column):
        return jnp.sum(jnp.where(eye, column, 0.0), axis=0, keepdims=True)

    flags = vbuf[:, 0, :].astype(jnp.float32)
    image_total = jnp.sum(jnp.sum(flags, axis=1, keepdims=True), axis=0, keepdims=True)
    starts = lax.broadcasted_iota(jnp.int32, (n, N), 1) * n
    lanes = lax.broadcasted_iota(jnp.int32, (n, n), 1)

    def caption_state(slot):
        target = to_column(posb[slot].astype(jnp.float32)).astype(jnp.int32)
        inside = (target >= starts) & (target < starts + n)
        picked = jnp.dot(
            jnp.where(inside, 1.0, 0.0).astype(jnp.bfloat16), flags.astype(jnp.bfloat16),
            preferred_element_type=jnp.float32,
        )
        start = jnp.sum(jnp.where(inside, starts, 0).astype(jnp.float32), axis=1, keepdims=True)
        low = target - start.astype(jnp.int32)
        ok = jnp.sum(jnp.where(lanes == low, picked, 0.0), axis=1, keepdims=True)
        return target, ok

    image_ok = jnp.concatenate(
        [vbuf[u * G + s].astype(jnp.float32) for s in range(G)], axis=1
    )
    image_ids = u * (G * n) + lax.broadcasted_iota(jnp.int32, (1, G * n), 1)
    colacc[0:1, :] = jnp.full((1, G * n), floor, jnp.float32)
    colacc[1:3, :] = jnp.zeros((2, G * n), jnp.float32)

    if U > 2:
        pass_on(1)
    for k in range(1, M):
        copy = relay_copy(k)
        copy.wait_recv()
        copy.start()
        if k == 2 and U > 2:
            pass_on(2)
    for d in range(2 if M <= 2 else 3, U - 1):
        pass_on(d)
    img_local.wait()
    cap_local.wait()
    for k in range(M):
        slot = partner if k == 0 else (same_core(k) // rep + 1 - 2 * core) * rep + same_core(k) % rep
        remote(
            img_ref, imgs.at[slot], own_send.at[0], img_sem.at[slot], member(u, partner)
        ).wait_recv()

    small = jnp.minimum(u, U - 1 - u)
    side = jnp.where(u < U - 1 - u, 1, -1)

    def slot_at(k):
        near = jnp.where(k % 2 == 1, u - (k + 1) // 2, u + (k + 1) // 2)
        return jnp.where(k <= 2 * small, near, u + side * (k - small))

    def row_copy(slot):
        return remote(
            rowsend.at[slot], rowrecv.at[u], row_send.at[slot], row_recv.at[u], member(slot, g)
        )

    @pl.loop(0, U)
    def _(k):
        slot = slot_at(k)

        @pl.when((slot - u == U - 1) | (u - slot == U - 1))
        def _():
            for p in range(PIECES):
                rows = pl.ds(p * ph, ph)
                remote(
                    caps.at[slot, rows], caps.at[slot, rows], up_sem.at[slot * PIECES + p],
                    cap_sem.at[slot * PIECES + p], member(slot, g),
                ).wait_recv()

        target, ok = caption_state(slot)
        scores = lax.dot_general(
            caps[slot], imgs[...].reshape(G * n, imgs.shape[2]), (((1,), (1,)), ((), ())),
            preferred_element_type=jnp.float32,
        )
        usable = jnp.where(image_ok > 0, scores, very_low)
        row_peak = jnp.maximum(jnp.max(usable, axis=1, keepdims=True), floor)
        row_total = jnp.sum(jnp.exp(usable - row_peak), axis=1, keepdims=True)
        picked = jnp.where(target == image_ids, scores, 0.0)
        row_match = jnp.sum(picked, axis=1, keepdims=True)
        rowsend[slot, 0:1, :] = to_row(row_peak)
        rowsend[slot, 1:2, :] = to_row(row_total)
        rowsend[slot, 2:3, :] = to_row(row_match)

        @pl.when(slot != u)
        def _():
            row_copy(slot).start()

        live = jnp.where(ok > 0, scores, very_low)
        old_peak = colacc[0:1, :]
        peak = jnp.maximum(jnp.max(live, axis=0, keepdims=True), old_peak)
        total = jnp.sum(jnp.exp(live - peak), axis=0, keepdims=True)
        colacc[1:2, :] = colacc[1:2, :] * jnp.exp(old_peak - peak) + total
        colacc[0:1, :] = peak
        colacc[2:3, :] = colacc[2:3, :] + jnp.sum(picked, axis=0, keepdims=True)

    for s in range(G):
        colsend[s, 0:3, :] = colacc[0:3, s * n : (s + 1) * n]

    def col_copy(k):
        slot = (g + k) % G
        return remote(
            colsend.at[slot], colrecv.at[g], col_send.at[k], col_recv.at[g], member(u, slot)
        )

    for k in range(1, G):
        col_copy(k).start()

    rowrecv[u] = rowsend[u]
    colrecv[g] = colsend[g]
    own_target, own_caption_ok = caption_state(u)
    caption_ok = to_row(own_caption_ok)

    def joined(parts, count):
        peak = parts[0, 0:1, :]
        for s in range(1, count):
            peak = jnp.maximum(peak, parts[s, 0:1, :])
        total = jnp.zeros_like(peak)
        match = jnp.zeros_like(peak)
        for s in range(count):
            total += parts[s, 1:2, :] * jnp.exp(parts[s, 0:1, :] - peak)
            match += parts[s, 2:3, :]
        return peak + jnp.log(total) - match

    for k in range(1, U):
        slot = (u + k) % U
        remote(
            rowsend.at[slot], rowrecv.at[slot], row_send.at[slot], row_recv.at[slot],
            member(slot, g),
        ).wait_recv()
    caption_loss = caption_ok * joined(rowrecv, U)
    closs_ref[...] = caption_loss
    for k in range(1, G):
        slot = (g + k) % G
        remote(
            colsend.at[slot], colrecv.at[slot], col_send.at[k], col_recv.at[slot],
            member(u, slot),
        ).wait_recv()
    image_loss = val_ref[...].astype(jnp.float32) * joined(colrecv, G)
    iloss_ref[...] = image_loss
    own_sum = jnp.sum(caption_loss + image_loss, axis=1, keepdims=True)
    part[me] = jnp.broadcast_to(own_sum, (1, 128))

    def part_copy(k):
        return remote(
            part.at[me], part.at[me], part_send.at[k], part_recv.at[me], device((me + k) % N)
        )

    @pl.loop(1, N)
    def _(k):
        part_copy(k).start()

    for d in range(U - 1):
        for p in range(PIECES):
            @pl.when((u - d >= 0) & (u < U - 1))
            def _():
                cap_copy(u - d, p, True).wait_send()

            @pl.when((u + d < U) & (u > 0))
            def _():
                cap_copy(u + d, p, False).wait_send()

    for k in range(M):
        own_img_copy(k).wait_send()
        if k:
            relay_copy(k).wait_send()
    for k in range(1, U):
        pos_copy(k).wait_send()
        row_copy((u + k) % U).wait_send()
    for k in range(1, G):
        col_copy(k).wait_send()

    @pl.loop(1, N)
    def _(k):
        val_copy(k).wait_send()

    @pl.loop(1, N)
    def _(k):
        slot = (me + k) % N
        remote(
            part.at[slot], part.at[slot], part_send.at[k], part_recv.at[slot], device(slot)
        ).wait_recv()

    whole = jnp.sum(part[:, 0, :], axis=0, keepdims=True)
    loss_ref[...] = whole[:, 0:1] / (2.0 * image_total)

    @pl.loop(1, N)
    def _(k):
        part_copy(k).wait_send()


def local(blk, rep, captions, images, positives, valid):
    n, width = captions.shape
    U, V = grid_of(blk, rep)
    N = blk * rep
    G = N // U
    f32, i32 = jnp.float32, jnp.int32
    dma = lambda count: pltpu.SemaphoreType.DMA((count,))
    vmem = pl.BlockSpec(memory_space=pltpu.VMEM)
    caption_loss, image_loss, loss = pl.pallas_call(
        functools.partial(kernel, blk, rep),
        out_shape=(
            jax.ShapeDtypeStruct((1, n), f32),
            jax.ShapeDtypeStruct((1, n), f32),
            jax.ShapeDtypeStruct((1, 1), f32),
        ),
        in_specs=[vmem] * 4,
        out_specs=(vmem,) * 3,
        scratch_shapes=[
            pltpu.VMEM((U, n, width), captions.dtype),
            pltpu.VMEM((G, n, width), images.dtype),
            pltpu.VMEM((U, 1, n), i32),
            pltpu.VMEM((N, 1, n), i32),
            pltpu.VMEM((U, 8, n), f32),
            pltpu.VMEM((U, 8, n), f32),
            pltpu.VMEM((G, 8, n), f32),
            pltpu.VMEM((G, 8, n), f32),
            pltpu.VMEM((N, 1, 128), f32),
            pltpu.VMEM((8, G * n), f32),
            dma(2), dma(U * PIECES), dma(U * PIECES), dma(U * PIECES),
            dma(U), dma(U), dma(N), dma(N),
            dma(V * rep), dma(V * rep), dma(G),
            dma(U), dma(U), dma(G), dma(G), dma(N), dma(N),
        ],
        compiler_params=pltpu.CompilerParams(collective_id=0, has_side_effects=True),
    )(captions, images, positives.reshape(1, n), valid.reshape(1, n))
    return caption_loss.reshape(n), image_loss.reshape(n), loss.reshape(())


def solution(mesh):
    placed = (
        P(("blk", "rep"), None),
        P(("blk", "rep"), None),
        P(("blk", "rep")),
        P(("blk", "rep")),
    )
    return jax.shard_map(
        functools.partial(local, mesh.shape["blk"], mesh.shape["rep"]),
        mesh=mesh,
        in_specs=placed,
        out_specs=(P(("blk", "rep")), P(("blk", "rep")), P()),
        check_vma=False,
    )
```

```python
import functools

import jax
import jax.numpy as jnp
from jax import lax
from jax.experimental import pallas as pl
from jax.experimental.pallas import tpu as pltpu
from jax.sharding import PartitionSpec as P

very_low = -1e30
floor = -1e29
PIECES = 2


def grid_of(blk, rep):
    chips = (blk // 2) * rep
    planes = 1
    while (planes * 2) ** 2 <= chips and (blk // 2) % (planes * 2) == 0:
        planes *= 2
    return planes, blk // 2 // planes


def mod(a, b):
    return a & (b - 1) if b & (b - 1) == 0 else lax.rem(a, b)


def div(a, b):
    return a >> (b.bit_length() - 1) if b & (b - 1) == 0 else lax.div(a, b)


def kernel(
    blk, rep, cap_ref, img_ref, pos_ref, val_ref, closs_ref, iloss_ref, loss_ref,
    caps, imgs, posb, vbuf, rowsend, rowrecv, colsend, colrecv, part, colacc,
    loc_sem, up_sem, down_sem, cap_sem, pos_send, pos_recv, val_send, val_recv, plane_send, plane_recv,
    own_send, relay_send, corner_send, img_sem, row_send, row_recv, col_send, col_recv, part_send, part_recv,
):
    U, V = grid_of(blk, rep)
    N = blk * rep
    G = N // U
    n = cap_ref.shape[0]
    ph = n // PIECES
    b, r = lax.axis_index("blk"), lax.axis_index("rep")
    core = mod(b, 2)
    u = div(b, 2 * V)
    v = mod(div(b, 2), V)
    me = b * rep + r
    g = mod(me, G)

    def member(uu, gg):
        return uu * G + gg

    def remote(src, dst, ss, rs, to):
        return pltpu.make_async_remote_copy(
            src_ref=src, dst_ref=dst, send_sem=ss, recv_sem=rs, device_id=to,
            device_id_type=pl.DeviceIdType.LOGICAL,
        )

    barrier = pltpu.get_barrier_semaphore()

    near = [member(u, mod(g + k, G)) for k in range(1, G)]
    near += [member(mod(u + k, U), g) for k in range(1, U)]
    for to in near:
        pl.semaphore_signal(
            barrier, inc=1, device_id=to, device_id_type=pl.DeviceIdType.LOGICAL
        )
    pl.semaphore_wait(barrier, len(near))

    def cap_copy(slot, p, up):
        rows = pl.ds(p * ph, ph)
        to = member(u + 1 if up else u - 1, g)
        return remote(
            caps.at[slot, rows], caps.at[slot, rows],
            (up_sem if up else down_sem).at[slot * PIECES + p], cap_sem.at[slot * PIECES + p], to,
        )

    def own_cap_copy(p, up):
        rows = pl.ds(p * ph, ph)
        to = member(u + 1 if up else u - 1, g)
        return remote(
            cap_ref.at[rows], caps.at[u, rows],
            (up_sem if up else down_sem).at[u * PIECES + p], cap_sem.at[u * PIECES + p], to,
        )

    for p in range(PIECES):
        @pl.when(u < U - 1)
        def _():
            own_cap_copy(p, True).start()

        @pl.when(u > 0)
        def _():
            own_cap_copy(p, False).start()

    def same_core(k):
        vv, rr = mod(v + k // rep, V), mod(r + k % rep, rep)
        return (vv * 2 + core) * rep + rr

    partner = (v * 2 + 1 - core) * rep + r
    M = V * rep

    def own_img_copy(k):
        to = partner if k == 0 else same_core(k)
        return remote(img_ref, imgs.at[g], own_send.at[k], img_sem.at[g], member(u, to))

    def relay_copy(k):
        slot = same_core(k)
        return remote(
            imgs.at[slot], imgs.at[slot], relay_send.at[k], img_sem.at[slot], member(u, partner)
        )

    sides = [k for k in range(1, M) if k < rep or k % rep == 0]
    corners = [k for k in range(1, M) if k not in sides]

    def corner_copy(k, half):
        if half == 0:
            slot, to = same_core(k - k % rep), same_core(k % rep)
        else:
            slot, to = same_core(k % rep), same_core(k - k % rep)
        rows = pl.ds(half * (n // 2), n // 2)
        return remote(
            imgs.at[slot, rows], imgs.at[slot, rows], corner_send.at[half * M + k],
            img_sem.at[half * G + slot], member(u, to),
        )

    def corner_arrival(k, half):
        slot = same_core(k)
        rows = pl.ds(half * (n // 2), n // 2)
        return remote(
            imgs.at[slot, rows], imgs.at[slot, rows], corner_send.at[half * M + k],
            img_sem.at[half * G + slot], member(u, slot),
        )

    for k in sides + [0]:
        own_img_copy(k).start()

    def pos_copy(k):
        return remote(
            pos_ref, posb.at[u], pos_send.at[k], pos_recv.at[u], member(mod(u + k, U), g)
        )

    for k in range(1, U):
        pos_copy(k).start()

    def val_copy(k):
        return remote(
            val_ref, vbuf.at[me], val_send.at[k], val_recv.at[g], member(u, mod(g + k, G))
        )

    for k in range(1, G):
        val_copy(k).start()

    def plane_copy(k):
        rows = pl.ds(u * G, G)
        return remote(
            vbuf.at[rows], vbuf.at[rows], plane_send.at[k], plane_recv.at[u],
            member(mod(u + k, U), g),
        )

    cap_local = pltpu.make_async_copy(cap_ref, caps.at[u], loc_sem.at[0])
    img_local = pltpu.make_async_copy(img_ref, imgs.at[g], loc_sem.at[1])
    cap_local.start()
    img_local.start()
    posb[u] = pos_ref[...]
    vbuf[me] = val_ref[...]

    def pass_on(distance):
        for p in range(PIECES):
            @pl.when(u - distance >= 0)
            def _():
                copy = cap_copy(u - distance, p, True)
                copy.wait_recv()

                @pl.when(u < U - 1)
                def _():
                    copy.start()

            @pl.when(u + distance < U)
            def _():
                copy = cap_copy(u + distance, p, False)
                copy.wait_recv()

                @pl.when(u > 0)
                def _():
                    copy.start()

    for k in range(1, G):
        slot = mod(g + k, G)
        remote(
            val_ref, vbuf.at[u * G + slot], val_send.at[k], val_recv.at[slot], member(u, slot)
        ).wait_recv()
    for k in range(1, U):
        plane_copy(k).start()
    if U > 2:
        pass_on(1)
    for k in range(1, U):
        slot = mod(u + k, U)
        rows = pl.ds(slot * G, G)
        remote(
            vbuf.at[rows], vbuf.at[rows], plane_send.at[k], plane_recv.at[slot], member(slot, g)
        ).wait_recv()
    for k in range(1, U):
        slot = mod(u + k, U)
        remote(
            pos_ref, posb.at[slot], pos_send.at[k], pos_recv.at[slot], member(slot, g)
        ).wait_recv()

    eye = lax.broadcasted_iota(jnp.int32, (n, n), 0) == lax.broadcasted_iota(jnp.int32, (n, n), 1)

    def to_column(row):
        return jnp.sum(jnp.where(eye, row, 0.0), axis=1, keepdims=True)

    def to_row(column):
        return jnp.sum(jnp.where(eye, column, 0.0), axis=0, keepdims=True)

    flags = vbuf[:, 0, :].astype(jnp.float32)
    image_total = jnp.sum(jnp.sum(flags, axis=1, keepdims=True), axis=0, keepdims=True)
    starts = lax.broadcasted_iota(jnp.int32, (n, N), 1) * n
    lanes = lax.broadcasted_iota(jnp.int32, (n, n), 1)

    def caption_state(slot):
        target = to_column(posb[slot].astype(jnp.float32)).astype(jnp.int32)
        inside = (target >= starts) & (target < starts + n)
        picked = jnp.dot(
            jnp.where(inside, 1.0, 0.0).astype(jnp.bfloat16), flags.astype(jnp.bfloat16),
            preferred_element_type=jnp.float32,
        )
        start = jnp.sum(jnp.where(inside, starts, 0).astype(jnp.float32), axis=1, keepdims=True)
        low = target - start.astype(jnp.int32)
        ok = jnp.sum(jnp.where(lanes == low, picked, 0.0), axis=1, keepdims=True)
        return target, ok

    image_ok = jnp.concatenate(
        [vbuf[u * G + s].astype(jnp.float32) for s in range(G)], axis=1
    )
    image_ids = u * (G * n) + lax.broadcasted_iota(jnp.int32, (1, G * n), 1)
    colacc[0:1, :] = jnp.full((1, G * n), floor, jnp.float32)
    colacc[1:3, :] = jnp.zeros((2, G * n), jnp.float32)

    for k in sides:
        copy = relay_copy(k)
        copy.wait_recv()
        for c in corners:
            if k == c - c % rep:
                corner_copy(c, 0).start()
            if k == c % rep:
                corner_copy(c, 1).start()
        copy.start()
    for d in range(2, U - 1):
        pass_on(d)
    for k in corners:
        corner_arrival(k, 0).wait_recv()
        corner_arrival(k, 1).wait_recv()
        relay_copy(k).start()
    img_local.wait()
    cap_local.wait()
    for k in range(M):
        slot = partner if k == 0 else same_core(k) + (1 - 2 * core) * rep
        remote(
            img_ref, imgs.at[slot], own_send.at[0], img_sem.at[slot], member(u, partner)
        ).wait_recv()

    small = jnp.minimum(u, U - 1 - u)
    side = jnp.where(u < U - 1 - u, 1, -1)

    def slot_at(k):
        near = jnp.where(mod(k, 2) == 1, u - div(k + 1, 2), u + div(k + 1, 2))
        return jnp.where(k <= 2 * small, near, u + side * (k - small))

    def row_copy(slot):
        return remote(
            rowsend.at[slot], rowrecv.at[u], row_send.at[slot], row_recv.at[u], member(slot, g)
        )

    @pl.loop(0, U)
    def _(k):
        slot = slot_at(k)

        @pl.when((slot - u == U - 1) | (u - slot == U - 1))
        def _():
            for p in range(PIECES):
                rows = pl.ds(p * ph, ph)
                remote(
                    caps.at[slot, rows], caps.at[slot, rows], up_sem.at[slot * PIECES + p],
                    cap_sem.at[slot * PIECES + p], member(slot, g),
                ).wait_recv()

        target, ok = caption_state(slot)
        scores = lax.dot_general(
            caps[slot], imgs[...].reshape(G * n, imgs.shape[2]), (((1,), (1,)), ((), ())),
            preferred_element_type=jnp.float32,
        )
        usable = jnp.where(image_ok > 0, scores, very_low)
        row_peak = jnp.maximum(jnp.max(usable, axis=1, keepdims=True), floor)
        row_total = jnp.sum(jnp.exp(usable - row_peak), axis=1, keepdims=True)
        picked = jnp.where(target == image_ids, scores, 0.0)
        row_match = jnp.sum(picked, axis=1, keepdims=True)
        rowsend[slot, 0:1, :] = to_row(row_peak)
        rowsend[slot, 1:2, :] = to_row(row_total)
        rowsend[slot, 2:3, :] = to_row(row_match)

        @pl.when(slot != u)
        def _():
            row_copy(slot).start()

        live = jnp.where(ok > 0, scores, very_low)
        old_peak = colacc[0:1, :]
        peak = jnp.maximum(jnp.max(live, axis=0, keepdims=True), old_peak)
        total = jnp.sum(jnp.exp(live - peak), axis=0, keepdims=True)
        colacc[1:2, :] = colacc[1:2, :] * jnp.exp(old_peak - peak) + total
        colacc[0:1, :] = peak
        colacc[2:3, :] = colacc[2:3, :] + jnp.sum(picked, axis=0, keepdims=True)

    for s in range(G):
        colsend[s, 0:3, :] = colacc[0:3, s * n : (s + 1) * n]

    def col_copy(k):
        slot = mod(g + k, G)
        return remote(
            colsend.at[slot], colrecv.at[g], col_send.at[k], col_recv.at[g], member(u, slot)
        )

    for k in range(1, G):
        col_copy(k).start()

    rowrecv[u] = rowsend[u]
    colrecv[g] = colsend[g]
    own_target, own_caption_ok = caption_state(u)
    caption_ok = to_row(own_caption_ok)

    def joined(parts, count):
        peak = parts[0, 0:1, :]
        for s in range(1, count):
            peak = jnp.maximum(peak, parts[s, 0:1, :])
        total = jnp.zeros_like(peak)
        match = jnp.zeros_like(peak)
        for s in range(count):
            total += parts[s, 1:2, :] * jnp.exp(parts[s, 0:1, :] - peak)
            match += parts[s, 2:3, :]
        return peak + jnp.log(total) - match

    for k in range(1, U):
        slot = mod(u + k, U)
        remote(
            rowsend.at[slot], rowrecv.at[slot], row_send.at[slot], row_recv.at[slot],
            member(slot, g),
        ).wait_recv()
    caption_loss = caption_ok * joined(rowrecv, U)
    closs_ref[...] = caption_loss
    for k in range(1, G):
        slot = mod(g + k, G)
        remote(
            colsend.at[slot], colrecv.at[slot], col_send.at[k], col_recv.at[slot],
            member(u, slot),
        ).wait_recv()
    image_loss = val_ref[...].astype(jnp.float32) * joined(colrecv, G)
    iloss_ref[...] = image_loss
    own_sum = jnp.sum(caption_loss + image_loss, axis=1, keepdims=True)
    part[me] = jnp.broadcast_to(own_sum, (1, 128))

    def part_copy(k):
        return remote(
            part.at[me], part.at[me], part_send.at[k], part_recv.at[me], mod(me + k, N)
        )

    @pl.loop(1, N)
    def _(k):
        part_copy(k).start()

    for d in range(U - 1):
        for p in range(PIECES):
            @pl.when((u - d >= 0) & (u < U - 1))
            def _():
                cap_copy(u - d, p, True).wait_send()

            @pl.when((u + d < U) & (u > 0))
            def _():
                cap_copy(u + d, p, False).wait_send()

    for k in [0] + sides:
        own_img_copy(k).wait_send()
    for k in range(1, M):
        relay_copy(k).wait_send()
    for k in corners:
        corner_copy(k, 0).wait_send()
        corner_copy(k, 1).wait_send()
    for k in range(1, U):
        pos_copy(k).wait_send()
        row_copy(mod(u + k, U)).wait_send()
    for k in range(1, G):
        col_copy(k).wait_send()

    for k in range(1, G):
        val_copy(k).wait_send()
    for k in range(1, U):
        plane_copy(k).wait_send()

    @pl.loop(1, N)
    def _(k):
        slot = mod(me + k, N)
        remote(
            part.at[slot], part.at[slot], part_send.at[k], part_recv.at[slot], slot
        ).wait_recv()

    whole = jnp.sum(part[:, 0, :], axis=0, keepdims=True)
    loss_ref[...] = whole[:, 0:1] / (2.0 * image_total)

    @pl.loop(1, N)
    def _(k):
        part_copy(k).wait_send()


def local(blk, rep, captions, images, positives, valid):
    n, width = captions.shape
    U, V = grid_of(blk, rep)
    N = blk * rep
    G = N // U
    f32, i32 = jnp.float32, jnp.int32
    dma = lambda count: pltpu.SemaphoreType.DMA((count,))
    vmem = pl.BlockSpec(memory_space=pltpu.VMEM)
    caption_loss, image_loss, loss = pl.pallas_call(
        functools.partial(kernel, blk, rep),
        out_shape=(
            jax.ShapeDtypeStruct((1, n), f32),
            jax.ShapeDtypeStruct((1, n), f32),
            jax.ShapeDtypeStruct((1, 1), f32),
        ),
        in_specs=[vmem] * 4,
        out_specs=(vmem,) * 3,
        scratch_shapes=[
            pltpu.VMEM((U, n, width), captions.dtype),
            pltpu.VMEM((G, n, width), images.dtype),
            pltpu.VMEM((U, 1, n), i32),
            pltpu.VMEM((N, 1, n), i32),
            pltpu.VMEM((U, 8, n), f32),
            pltpu.VMEM((U, 8, n), f32),
            pltpu.VMEM((G, 8, n), f32),
            pltpu.VMEM((G, 8, n), f32),
            pltpu.VMEM((N, 1, 128), f32),
            pltpu.VMEM((8, G * n), f32),
            dma(2), dma(U * PIECES), dma(U * PIECES), dma(U * PIECES),
            dma(U), dma(U), dma(G), dma(G), dma(U), dma(U),
            dma(V * rep), dma(V * rep), dma(2 * V * rep), dma(2 * G),
            dma(U), dma(U), dma(G), dma(G), dma(N), dma(N),
        ],
        compiler_params=pltpu.CompilerParams(collective_id=0, has_side_effects=True),
    )(captions, images, positives.reshape(1, n), valid.reshape(1, n))
    return caption_loss.reshape(n), image_loss.reshape(n), loss.reshape(())


def solution(mesh):
    placed = (
        P(("blk", "rep"), None),
        P(("blk", "rep"), None),
        P(("blk", "rep")),
        P(("blk", "rep")),
    )
    return jax.shard_map(
        functools.partial(local, mesh.shape["blk"], mesh.shape["rep"]),
        mesh=mesh,
        in_specs=placed,
        out_specs=(P(("blk", "rep")), P(("blk", "rep")), P()),
        check_vma=False,
    )
```

```python
import functools

import jax
import jax.numpy as jnp
from jax import lax
from jax.experimental import pallas as pl
from jax.experimental.pallas import tpu as pltpu
from jax.sharding import PartitionSpec as P

very_low = -1e30
floor = -1e29
PIECES = 2


def grid_of(blk, rep):
    chips = (blk // 2) * rep
    planes = 1
    while (planes * 2) ** 2 <= chips and (blk // 2) % (planes * 2) == 0:
        planes *= 2
    return planes, blk // 2 // planes


def mod(a, b):
    return a & (b - 1) if b & (b - 1) == 0 else lax.rem(a, b)


def div(a, b):
    return a >> (b.bit_length() - 1) if b & (b - 1) == 0 else lax.div(a, b)


def kernel(
    blk, rep, cap_ref, img_ref, pos_ref, val_ref, closs_ref, iloss_ref, loss_ref,
    caps, imgs, posb, vbuf, rowsend, rowrecv, colsend, colrecv, part, colacc,
    loc_sem, up_sem, down_sem, cap_sem, pos_send, pos_recv, val_send, val_recv, plane_send, plane_recv,
    own_send, relay_send, corner_send, img_sem, row_send, row_recv, col_send, col_recv, part_send, part_recv,
):
    U, V = grid_of(blk, rep)
    N = blk * rep
    G = N // U
    n = cap_ref.shape[0]
    ph = n // PIECES
    b, r = lax.axis_index("blk"), lax.axis_index("rep")
    core = mod(b, 2)
    u = div(b, 2 * V)
    v = mod(div(b, 2), V)
    me = b * rep + r
    g = mod(me, G)

    def member(uu, gg):
        return uu * G + gg

    def remote(src, dst, ss, rs, to):
        return pltpu.make_async_remote_copy(
            src_ref=src, dst_ref=dst, send_sem=ss, recv_sem=rs, device_id=to,
            device_id_type=pl.DeviceIdType.LOGICAL,
        )

    barrier = pltpu.get_barrier_semaphore()

    near = [member(u, mod(g + k, G)) for k in range(1, G)]
    near += [member(mod(u + k, U), g) for k in range(1, U)]
    for to in near:
        pl.semaphore_signal(
            barrier, inc=1, device_id=to, device_id_type=pl.DeviceIdType.LOGICAL
        )
    pl.semaphore_wait(barrier, len(near))

    def cap_copy(slot, p, up):
        rows = pl.ds(p * ph, ph)
        to = member(u + 1 if up else u - 1, g)
        return remote(
            caps.at[slot, rows], caps.at[slot, rows],
            (up_sem if up else down_sem).at[slot * PIECES + p], cap_sem.at[slot * PIECES + p], to,
        )

    def own_cap_copy(p, up):
        rows = pl.ds(p * ph, ph)
        to = member(u + 1 if up else u - 1, g)
        return remote(
            cap_ref.at[rows], caps.at[u, rows],
            (up_sem if up else down_sem).at[u * PIECES + p], cap_sem.at[u * PIECES + p], to,
        )

    def pos_copy(k):
        return remote(
            pos_ref, posb.at[u], pos_send.at[k], pos_recv.at[u], member(mod(u + k, U), g)
        )

    for k in range(1, U):
        pos_copy(k).start()

    def val_copy(k):
        return remote(
            val_ref, vbuf.at[me], val_send.at[k], val_recv.at[g], member(u, mod(g + k, G))
        )

    for k in range(1, G):
        val_copy(k).start()

    def plane_copy(k):
        rows = pl.ds(u * G, G)
        return remote(
            vbuf.at[rows], vbuf.at[rows], plane_send.at[k], plane_recv.at[u],
            member(mod(u + k, U), g),
        )

    for p in range(PIECES):
        @pl.when(u < U - 1)
        def _():
            own_cap_copy(p, True).start()

        @pl.when(u > 0)
        def _():
            own_cap_copy(p, False).start()

    def same_core(k):
        vv, rr = mod(v + k // rep, V), mod(r + k % rep, rep)
        return (vv * 2 + core) * rep + rr

    partner = (v * 2 + 1 - core) * rep + r
    M = V * rep

    def own_img_copy(k):
        to = partner if k == 0 else same_core(k)
        return remote(img_ref, imgs.at[g], own_send.at[k], img_sem.at[g], member(u, to))

    def relay_copy(k):
        slot = same_core(k)
        return remote(
            imgs.at[slot], imgs.at[slot], relay_send.at[k], img_sem.at[slot], member(u, partner)
        )

    sides = [k for k in range(1, M) if k < rep or k % rep == 0]
    corners = [k for k in range(1, M) if k not in sides]

    def corner_copy(k, half):
        if half == 0:
            slot, to = same_core(k - k % rep), same_core(k % rep)
        else:
            slot, to = same_core(k % rep), same_core(k - k % rep)
        rows = pl.ds(half * (n // 2), n // 2)
        return remote(
            imgs.at[slot, rows], imgs.at[slot, rows], corner_send.at[half * M + k],
            img_sem.at[half * G + slot], member(u, to),
        )

    def corner_arrival(k, half):
        slot = same_core(k)
        rows = pl.ds(half * (n // 2), n // 2)
        return remote(
            imgs.at[slot, rows], imgs.at[slot, rows], corner_send.at[half * M + k],
            img_sem.at[half * G + slot], member(u, slot),
        )

    for k in sides + [0]:
        own_img_copy(k).start()

    cap_local = pltpu.make_async_copy(cap_ref, caps.at[u], loc_sem.at[0])
    img_local = pltpu.make_async_copy(img_ref, imgs.at[g], loc_sem.at[1])
    cap_local.start()
    img_local.start()
    posb[u] = pos_ref[...]
    vbuf[me] = val_ref[...]

    def pass_on(distance):
        for p in range(PIECES):
            @pl.when(u - distance >= 0)
            def _():
                copy = cap_copy(u - distance, p, True)
                copy.wait_recv()

                @pl.when(u < U - 1)
                def _():
                    copy.start()

            @pl.when(u + distance < U)
            def _():
                copy = cap_copy(u + distance, p, False)
                copy.wait_recv()

                @pl.when(u > 0)
                def _():
                    copy.start()

    for k in range(1, G):
        slot = mod(g + k, G)
        remote(
            val_ref, vbuf.at[u * G + slot], val_send.at[k], val_recv.at[slot], member(u, slot)
        ).wait_recv()
    for k in range(1, U):
        plane_copy(k).start()
    if U > 2:
        pass_on(1)
    for k in sides:
        copy = relay_copy(k)
        copy.wait_recv()
        for c in corners:
            if k == c - c % rep:
                corner_copy(c, 0).start()
            if k == c % rep:
                corner_copy(c, 1).start()
        copy.start()
    for d in range(2, U - 1):
        pass_on(d)
    for k in corners:
        corner_arrival(k, 0).wait_recv()
        corner_arrival(k, 1).wait_recv()
        relay_copy(k).start()
    for k in range(1, U):
        slot = mod(u + k, U)
        rows = pl.ds(slot * G, G)
        remote(
            vbuf.at[rows], vbuf.at[rows], plane_send.at[k], plane_recv.at[slot], member(slot, g)
        ).wait_recv()
    for k in range(1, U):
        slot = mod(u + k, U)
        remote(
            pos_ref, posb.at[slot], pos_send.at[k], pos_recv.at[slot], member(slot, g)
        ).wait_recv()

    eye = lax.broadcasted_iota(jnp.int32, (n, n), 0) == lax.broadcasted_iota(jnp.int32, (n, n), 1)

    def to_column(row):
        return jnp.sum(jnp.where(eye, row, 0.0), axis=1, keepdims=True)

    def to_row(column):
        return jnp.sum(jnp.where(eye, column, 0.0), axis=0, keepdims=True)

    flags = vbuf[:, 0, :].astype(jnp.float32)
    image_total = jnp.sum(jnp.sum(flags, axis=1, keepdims=True), axis=0, keepdims=True)
    starts = lax.broadcasted_iota(jnp.int32, (n, N), 1) * n
    lanes = lax.broadcasted_iota(jnp.int32, (n, n), 1)

    def caption_state(slot):
        target = to_column(posb[slot].astype(jnp.float32)).astype(jnp.int32)
        inside = (target >= starts) & (target < starts + n)
        picked = jnp.dot(
            jnp.where(inside, 1.0, 0.0).astype(jnp.bfloat16), flags.astype(jnp.bfloat16),
            preferred_element_type=jnp.float32,
        )
        start = jnp.sum(jnp.where(inside, starts, 0).astype(jnp.float32), axis=1, keepdims=True)
        low = target - start.astype(jnp.int32)
        ok = jnp.sum(jnp.where(lanes == low, picked, 0.0), axis=1, keepdims=True)
        return target, ok

    image_ok = jnp.concatenate(
        [vbuf[u * G + s].astype(jnp.float32) for s in range(G)], axis=1
    )
    image_ids = u * (G * n) + lax.broadcasted_iota(jnp.int32, (1, G * n), 1)
    colacc[0:1, :] = jnp.full((1, G * n), floor, jnp.float32)
    colacc[1:3, :] = jnp.zeros((2, G * n), jnp.float32)

    img_local.wait()
    cap_local.wait()
    for k in range(M):
        slot = partner if k == 0 else same_core(k) + (1 - 2 * core) * rep
        remote(
            img_ref, imgs.at[slot], own_send.at[0], img_sem.at[slot], member(u, partner)
        ).wait_recv()

    small = jnp.minimum(u, U - 1 - u)
    side = jnp.where(u < U - 1 - u, 1, -1)

    def slot_at(k):
        near = jnp.where(mod(k, 2) == 1, u - div(k + 1, 2), u + div(k + 1, 2))
        return jnp.where(k <= 2 * small, near, u + side * (k - small))

    def row_copy(slot):
        return remote(
            rowsend.at[slot], rowrecv.at[u], row_send.at[slot], row_recv.at[u], member(slot, g)
        )

    @pl.loop(0, U)
    def _(k):
        slot = slot_at(k)

        @pl.when((slot - u == U - 1) | (u - slot == U - 1))
        def _():
            for p in range(PIECES):
                rows = pl.ds(p * ph, ph)
                remote(
                    caps.at[slot, rows], caps.at[slot, rows], up_sem.at[slot * PIECES + p],
                    cap_sem.at[slot * PIECES + p], member(slot, g),
                ).wait_recv()

        target, ok = caption_state(slot)
        scores = lax.dot_general(
            caps[slot], imgs[...].reshape(G * n, imgs.shape[2]), (((1,), (1,)), ((), ())),
            preferred_element_type=jnp.float32,
        )
        usable = jnp.where(image_ok > 0, scores, very_low)
        row_peak = jnp.maximum(jnp.max(usable, axis=1, keepdims=True), floor)
        row_total = jnp.sum(jnp.exp(usable - row_peak), axis=1, keepdims=True)
        picked = jnp.where(target == image_ids, scores, 0.0)
        row_match = jnp.sum(picked, axis=1, keepdims=True)
        rowsend[slot, 0:1, :] = to_row(row_peak)
        rowsend[slot, 1:2, :] = to_row(row_total)
        rowsend[slot, 2:3, :] = to_row(row_match)

        @pl.when(slot != u)
        def _():
            row_copy(slot).start()

        live = jnp.where(ok > 0, scores, very_low)
        old_peak = colacc[0:1, :]
        peak = jnp.maximum(jnp.max(live, axis=0, keepdims=True), old_peak)
        total = jnp.sum(jnp.exp(live - peak), axis=0, keepdims=True)
        colacc[1:2, :] = colacc[1:2, :] * jnp.exp(old_peak - peak) + total
        colacc[0:1, :] = peak
        colacc[2:3, :] = colacc[2:3, :] + jnp.sum(picked, axis=0, keepdims=True)

    for s in range(G):
        colsend[s, 0:3, :] = colacc[0:3, s * n : (s + 1) * n]

    def col_copy(k):
        slot = mod(g + k, G)
        return remote(
            colsend.at[slot], colrecv.at[g], col_send.at[k], col_recv.at[g], member(u, slot)
        )

    for k in range(1, G):
        col_copy(k).start()

    rowrecv[u] = rowsend[u]
    colrecv[g] = colsend[g]
    own_target, own_caption_ok = caption_state(u)
    caption_ok = to_row(own_caption_ok)

    def joined(parts, count):
        peak = parts[0, 0:1, :]
        for s in range(1, count):
            peak = jnp.maximum(peak, parts[s, 0:1, :])
        total = jnp.zeros_like(peak)
        match = jnp.zeros_like(peak)
        for s in range(count):
            total += parts[s, 1:2, :] * jnp.exp(parts[s, 0:1, :] - peak)
            match += parts[s, 2:3, :]
        return peak + jnp.log(total) - match

    for k in range(1, U):
        slot = mod(u + k, U)
        remote(
            rowsend.at[slot], rowrecv.at[slot], row_send.at[slot], row_recv.at[slot],
            member(slot, g),
        ).wait_recv()
    caption_loss = caption_ok * joined(rowrecv, U)
    closs_ref[...] = caption_loss
    for k in range(1, G):
        slot = mod(g + k, G)
        remote(
            colsend.at[slot], colrecv.at[slot], col_send.at[k], col_recv.at[slot],
            member(u, slot),
        ).wait_recv()
    image_loss = val_ref[...].astype(jnp.float32) * joined(colrecv, G)
    iloss_ref[...] = image_loss
    own_sum = jnp.sum(caption_loss + image_loss, axis=1, keepdims=True)
    part[me] = jnp.broadcast_to(own_sum, (1, 128))

    def part_copy(k):
        return remote(
            part.at[me], part.at[me], part_send.at[k], part_recv.at[me], mod(me + k, N)
        )

    @pl.loop(1, N)
    def _(k):
        part_copy(k).start()

    for d in range(U - 1):
        for p in range(PIECES):
            @pl.when((u - d >= 0) & (u < U - 1))
            def _():
                cap_copy(u - d, p, True).wait_send()

            @pl.when((u + d < U) & (u > 0))
            def _():
                cap_copy(u + d, p, False).wait_send()

    for k in [0] + sides:
        own_img_copy(k).wait_send()
    for k in range(1, M):
        relay_copy(k).wait_send()
    for k in corners:
        corner_copy(k, 0).wait_send()
        corner_copy(k, 1).wait_send()
    for k in range(1, U):
        pos_copy(k).wait_send()
        row_copy(mod(u + k, U)).wait_send()
    for k in range(1, G):
        col_copy(k).wait_send()

    for k in range(1, G):
        val_copy(k).wait_send()
    for k in range(1, U):
        plane_copy(k).wait_send()

    @pl.loop(1, N)
    def _(k):
        slot = mod(me + k, N)
        remote(
            part.at[slot], part.at[slot], part_send.at[k], part_recv.at[slot], slot
        ).wait_recv()

    whole = jnp.sum(part[:, 0, :], axis=0, keepdims=True)
    loss_ref[...] = whole[:, 0:1] / (2.0 * image_total)

    @pl.loop(1, N)
    def _(k):
        part_copy(k).wait_send()


def local(blk, rep, captions, images, positives, valid):
    n, width = captions.shape
    U, V = grid_of(blk, rep)
    N = blk * rep
    G = N // U
    f32, i32 = jnp.float32, jnp.int32
    dma = lambda count: pltpu.SemaphoreType.DMA((count,))
    vmem = pl.BlockSpec(memory_space=pltpu.VMEM)
    caption_loss, image_loss, loss = pl.pallas_call(
        functools.partial(kernel, blk, rep),
        out_shape=(
            jax.ShapeDtypeStruct((1, n), f32),
            jax.ShapeDtypeStruct((1, n), f32),
            jax.ShapeDtypeStruct((1, 1), f32),
        ),
        in_specs=[vmem] * 4,
        out_specs=(vmem,) * 3,
        scratch_shapes=[
            pltpu.VMEM((U, n, width), captions.dtype),
            pltpu.VMEM((G, n, width), images.dtype),
            pltpu.VMEM((U, 1, n), i32),
            pltpu.VMEM((N, 1, n), i32),
            pltpu.VMEM((U, 8, n), f32),
            pltpu.VMEM((U, 8, n), f32),
            pltpu.VMEM((G, 8, n), f32),
            pltpu.VMEM((G, 8, n), f32),
            pltpu.VMEM((N, 1, 128), f32),
            pltpu.VMEM((8, G * n), f32),
            dma(2), dma(U * PIECES), dma(U * PIECES), dma(U * PIECES),
            dma(U), dma(U), dma(G), dma(G), dma(U), dma(U),
            dma(V * rep), dma(V * rep), dma(2 * V * rep), dma(2 * G),
            dma(U), dma(U), dma(G), dma(G), dma(N), dma(N),
        ],
        compiler_params=pltpu.CompilerParams(collective_id=0, has_side_effects=True),
    )(captions, images, positives.reshape(1, n), valid.reshape(1, n))
    return caption_loss.reshape(n), image_loss.reshape(n), loss.reshape(())


def solution(mesh):
    placed = (
        P(("blk", "rep"), None),
        P(("blk", "rep"), None),
        P(("blk", "rep")),
        P(("blk", "rep")),
    )
    return jax.shard_map(
        functools.partial(local, mesh.shape["blk"], mesh.shape["rep"]),
        mesh=mesh,
        in_specs=placed,
        out_specs=(P(("blk", "rep")), P(("blk", "rep")), P()),
        check_vma=False,
    )
```
